128 devices in a mesh: tensor: 4 (over z_hi, core), dp: 32 (over y, x, z_lo).
Axes of the slice: x: 4, y: 4, z: 4 (z_hi: 2, z_lo: 2; z = z_hi * 2 + z_lo), core: 2. Of those that a mesh axis runs over, the one named last changes fastest.
Arguments:
- grads: bfloat16 [32, 4, 8192, 1024], P('dp', None, None, 'tensor'), may hold values from -6 to 6
- param: float32 [4, 8192, 1024], P(None, 'dp', 'tensor'), may hold values from -3 to 3
- q_m: bfloat16 [4, 8192, 1024], P(None, 'dp', 'tensor'), may hold values from -1 to 1
- m_scale: float32 [4], replicated, may hold values from 0.02 to 0.2
- q_v: bfloat16 [4, 8192, 1024], P(None, 'dp', 'tensor'), may hold values from 0.0009994507 to 1
- v_max: float32 [4, 8], P(None, 'tensor'), may hold values from 0.005 to 0.05
- v_exp: float32 [4, 8], P(None, 'tensor'), may hold values from 1 to 10
Outputs:
- new_param: float32 [4, 8192, 1024], P(None, 'dp', 'tensor')
- new_q_m: bfloat16 [4, 8192, 1024], P(None, 'dp', 'tensor')
- new_m_scale: float32 [4], replicated
- new_q_v: bfloat16 [4, 8192, 1024], P(None, 'dp', 'tensor')
- new_v_max: float32 [4, 8], P(None, 'tensor')
- new_v_exp: float32 [4, 8], P(None, 'tensor')
The draws below stay inside these ranges and needn't reach their ends.
All inputs are finite; a program needn't handle non-finite values. Where the reference program divides by a largest or mean magnitude, that divisor is 1e-20 or more.
Results may differ from the reference program's by a relative error of at most 0.001.
Values sent between devices are 32-bit elements; how exact they have to be, the bound alone decides.
No kernel may reach another device: no remote copies, remote signals or barrier semaphores. Data moves between devices by JAX's collectives and lax.ppermute only.
A program may use at most 192 MiB of HBM per device.

```python
import math
import jax
import jax.numpy as jnp
from jax import lax

D = 8192
KVW = 1024
HEAD = 128
TENSORS = 4
GROUPS = 8
REPLICAS = 32


def with_spikes(result, rng, source, target, parts, factor):
    def block_of(position):
        return (jnp.arange(result.shape[position]) // (result.shape[position] // parts)).reshape((-1,) + (1,) * (result.ndim - 1 - position))

    one_side = jax.random.permutation(rng, parts)[block_of(target)]
    second = (block_of(target) + parts // 2) % parts
    return jnp.where((block_of(source) == one_side) | (block_of(source) == second), factor * result, result)


def shard_levels(stream_key, dims, split, smallest, largest):
    loudness, own = 1.0, jax.random.fold_in(stream_key, 6)
    for axis_at, shards_of in split:
        steps = jnp.exp(jax.random.uniform(jax.random.fold_in(own, axis_at), (shards_of,), jnp.float32, smallest / len(split), largest / len(split)))
        loudness = loudness * jnp.repeat(steps, dims[axis_at] // shards_of).reshape([-1 if axis == axis_at else 1 for axis in range(len(dims))])
    return loudness


def gaussian(rng, shape, deviation, most, pieces=(), kind=jnp.bfloat16):
    values = jax.random.normal(rng, shape, jnp.float32) * deviation
    if len(pieces) > 0:
        values = shard_levels(rng, shape, pieces, -0.22, 0.18) * values
    return jnp.clip(values, min=-most, max=most).astype(kind)


def heavy_noise(stream_key, shape, scale, most, split, heavy, dtype=jnp.bfloat16):
    values = scale * jax.random.normal(stream_key, shape, jnp.float32)
    if split:
        values = values * shard_levels(stream_key, shape, split, -0.22, 0.18)
    return jnp.clip(with_spikes(values, jax.random.fold_in(stream_key, 3), *heavy), -most, most).astype(dtype)


def setup_inputs(seed: int = 0) -> dict:
    streams_of = jax.random.split(jax.random.key(seed), 8)
    return {
        "grads": heavy_noise(streams_of[0], (REPLICAS, TENSORS, D, KVW), 1.0, 6.0, ((0, 32), (3, 4)), (0, 2, 32, 2.75)),
        "param": gaussian(streams_of[1], (TENSORS, D, KVW), 0.5, 3.0, ((1, 32), (2, 4)), jnp.float32),
        "q_m": jnp.clip(jax.random.uniform(streams_of[2], (TENSORS, D, KVW), jnp.float32, -1.0, 1.0) * shard_levels(streams_of[2], (TENSORS, D, KVW), ((1, 32), (2, 4)), -0.4, 0.0), -1.0, 1.0).astype(jnp.bfloat16),
        "m_scale": jnp.clip(jnp.exp(jax.random.uniform(streams_of[3], (TENSORS,), jnp.float32, math.log(0.02), math.log(0.2))), 0.02, 0.2),
        "q_v": jnp.clip(jnp.exp(math.log(1.0) - 6.9083047 * jax.random.uniform(streams_of[4], (TENSORS, D, KVW), jnp.float32) ** shard_levels(streams_of[4], (TENSORS, D, KVW), ((1, 32), (2, 4)), -0.2, 0.2)), 0.0009994507, 1.0).astype(jnp.bfloat16),
        "v_max": jnp.clip(jnp.exp(math.log(0.05) - 2.3025851 * jax.random.uniform(streams_of[5], (TENSORS, GROUPS), jnp.float32) ** shard_levels(streams_of[5], (TENSORS, GROUPS), ((1, 4),), -0.2, 0.2)), 0.005, 0.05),
        "v_exp": jnp.clip(1.0 + 9.0 * jax.random.uniform(streams_of[6], (TENSORS, GROUPS), jnp.float32) ** shard_levels(streams_of[6], (TENSORS, GROUPS), ((1, 4),), -0.2, 0.2), 1.0, 10.0),
    }


def reference(grads, param, q_m, m_scale, q_v, v_max, v_exp):

    def add_one(index, total):
        return total + lax.dynamic_index_in_dim(grads, index, 0, keepdims=False).astype(jnp.float32)
    summed = lax.fori_loop(0, REPLICAS, add_one, jnp.zeros((TENSORS, D, KVW), jnp.float32))
    grad = (summed / REPLICAS).reshape(TENSORS, D, GROUPS, HEAD)
    m_old = m_scale[:, None, None, None] * q_m.astype(jnp.float32).reshape(TENSORS, D, GROUPS, HEAD)
    stored = q_v.astype(jnp.float32).reshape(TENSORS, D, GROUPS, HEAD)
    v_old = v_max[:, None, :, None] * jnp.exp(jnp.log(stored) / v_exp[:, None, :, None])
    m_new = 0.9 * m_old + 0.1 * grad
    v_new = 0.95 * v_old + 0.05 * grad * grad
    weights = param.reshape(TENSORS, D, GROUPS, HEAD)
    new_param = weights - 0.02 * (m_new / (jnp.sqrt(v_new) + 1e-08) + 0.1 * weights)
    new_m_scale = lax.optimization_barrier(jnp.max(jnp.abs(m_new), axis=(1, 2, 3))) + 1e-06
    new_v_max = lax.optimization_barrier(jnp.max(v_new, axis=(1, 3)))
    v_low = lax.optimization_barrier(jnp.min(v_new, axis=(1, 3)))
    new_v_exp = 12.343 / jnp.maximum(jnp.log(new_v_max / v_low), 1.0)
    new_q_m = (m_new / new_m_scale[:, None, None, None]).astype(jnp.bfloat16)
    new_q_v = jnp.exp(new_v_exp[:, None, :, None] * jnp.log(v_new / new_v_max[:, None, :, None])).astype(jnp.bfloat16)
    shape = (TENSORS, D, KVW)
    return (new_param.reshape(shape), new_q_m.reshape(shape), new_m_scale, new_q_v.reshape(shape), new_v_max, new_v_exp)
```

```python
import jax
import jax.numpy as jnp
from jax import lax
from jax.sharding import Mesh
from jax.sharding import PartitionSpec as P

Y, X, Z = DP = ("dp_0", "dp_1", "dp_2")
EVERY = ("tensor", *DP)


def take(value, index, dim):
    return lax.dynamic_index_in_dim(value, index, dim, keepdims=False).astype(jnp.float32)


def shift(value, axis, by):
    n = lax.axis_size(axis)
    return lax.ppermute(value, axis, [(i, (i + by) % n) for i in range(n)])


def ring_sum(low, high, axis, dim):
    here = lax.axis_index(axis)

    def block(value, by):
        return take(value, (here + by) % 4, dim)

    far_up = shift(block(low, 2), axis, 1)
    far_down = shift(block(high, 2), axis, -1)
    near_up = shift(block(high, 1), axis, 1)
    near_down = shift(block(low, 3), axis, -1)
    full_up = shift(block(low, 1) + far_up, axis, 1)
    full_down = shift(block(high, 3) + far_down, axis, -1)
    return (
        block(low, 0) + near_down + full_up,
        block(high, 0) + near_up + full_down,
    )


def pair_sum(value, dim):
    here = lax.axis_index(Z)
    return take(value, here, dim) + shift(take(value, 1 - here, dim), Z, 1)


def sum_over_replicas(local, rows):
    count, _, width = local.shape
    part = rows // 4
    cells = local.reshape(count, 4, 4, 2, 4, part, width)
    late = count - 1
    pair = [pair_sum_early(cells[late], half) for half in range(2)]
    plane = []
    for half, (first, second) in enumerate(((Y, X), (X, Y))):
        dim = 1 if first == Y else 2
        low, high = (cells[:late, :, :, :, 2 * half + k] for k in range(2))
        low, high = ring_sum(low, high, first, dim)
        plane.append(ring_sum(low, high, second, 1))
    tail = []
    for half, (first, second) in enumerate(((Y, X), (X, Y))):
        low, high = pair[half]
        low, high = ring_sum(low, high, first, 0 if first == Y else 1)
        tail.append(ring_sum(low, high, second, 0))
    early = [pair_sum(piece, 1) for halves in plane for piece in halves]
    last = [piece for halves in tail for piece in halves]
    return jnp.concatenate(
        [jnp.concatenate(early, axis=1), jnp.concatenate(last, axis=0)[None]], axis=0
    )


def pair_sum_early(cells, half):
    here = lax.axis_index(Z)
    sent = take(cells[:, :, :, 2 * half : 2 * half + 2], 1 - here, 2)
    total = take(cells[:, :, :, 2 * half : 2 * half + 2], here, 2) + shift(sent, Z, 1)
    return total[:, :, 0], total[:, :, 1]


def from_everyone(value, axis):
    copies = jnp.broadcast_to(value, (lax.axis_size(axis), *value.shape))
    return lax.all_to_all(copies, axis, split_axis=0, concat_axis=0, tiled=True)


def extremes(peak, top, low):
    count, groups = top.shape
    flat = jnp.concatenate([peak, top.reshape(-1), -low.reshape(-1)])
    got = from_everyone(flat[None], EVERY).reshape(lax.axis_size("tensor"), -1, flat.size)
    own = jnp.max(take(got, lax.axis_index("tensor"), 0), axis=0)
    n = count * groups
    return (
        jnp.max(got[:, :, :count], axis=(0, 1)),
        own[count : count + n].reshape(count, groups),
        -own[count + n :].reshape(count, groups),
    )


def advance(summed, param, q_m, m_scale, q_v, v_max, v_exp, replicas):
    count, rows, width = q_m.shape
    groups = v_max.shape[1]
    shape4 = (count, rows, groups, width // groups)
    grad = (summed / replicas).reshape(shape4)
    m_old = m_scale[:, None, None, None] * q_m.astype(jnp.float32).reshape(shape4)
    stored = q_v.astype(jnp.float32).reshape(shape4)
    v_old = v_max[:, None, :, None] * jnp.exp(jnp.log(stored) / v_exp[:, None, :, None])
    m_new = 0.9 * m_old + 0.1 * grad
    v_new = 0.95 * v_old + 0.05 * grad * grad
    weights = param.reshape(shape4)
    new_param = weights - 0.02 * (m_new / (jnp.sqrt(v_new) + 1e-08) + 0.1 * weights)
    local_peak = jnp.max(jnp.abs(m_new), axis=(1, 2, 3))
    local_top = jnp.max(v_new, axis=(1, 3))
    local_low = jnp.min(v_new, axis=(1, 3))
    whole_top, group_top, group_low = extremes(local_peak, local_top, local_low)
    new_m_scale = whole_top + 1e-06
    new_v_exp = 12.343 / jnp.maximum(jnp.log(group_top / group_low), 1.0)
    new_q_m = (m_new / new_m_scale[:, None, None, None]).astype(jnp.bfloat16)
    new_q_v = jnp.exp(
        new_v_exp[:, None, :, None] * jnp.log(v_new / group_top[:, None, :, None])
    ).astype(jnp.bfloat16)
    flat = (count, rows, width)
    return (
        new_param.reshape(flat),
        new_q_m.reshape(flat),
        new_m_scale,
        new_q_v.reshape(flat),
        group_top,
        new_v_exp,
    )


def on_device(grads, param, q_m, m_scale, q_v, v_max, v_exp):
    replicas = lax.axis_size(DP)
    summed = sum_over_replicas(grads[0], q_m.shape[1])
    return advance(summed, param, q_m, m_scale, q_v, v_max, v_exp, replicas)


def solution(mesh):
    split = Mesh(
        mesh.devices.reshape(mesh.shape["tensor"], 4, 4, 2), ("tensor", "dp_0", "dp_1", "dp_2")
    )
    return jax.shard_map(
        on_device,
        mesh=split,
        in_specs=(
            P(DP, None, None, "tensor"),
            P(None, DP, "tensor"),
            P(None, DP, "tensor"),
            P(),
            P(None, DP, "tensor"),
            P(None, "tensor"),
            P(None, "tensor"),
        ),
        out_specs=(
            P(None, DP, "tensor"),
            P(None, DP, "tensor"),
            P(),
            P(None, DP, "tensor"),
            P(None, "tensor"),
            P(None, "tensor"),
        ),
        check_vma=False,
    )
```
